32 devices in a mesh: rows: 8 (over z, x), rep: 4 (over y, core).
Axes of the slice: x: 2, y: 2, z: 4, core: 2. Of those that a mesh axis runs over, the one named last changes fastest.
Arguments:
- embeddings: bfloat16 [32768, 1024], P(('rows', 'rep')), may hold values from -0.25 to 0.25
- assignments: int32 [32768], P(('rows', 'rep')), may hold values from 0 to 65535, as said below
- old_centroids: bfloat16 [65536, 1024], P('rows'), may hold values from -0.25 to 0.25
- prior_counts: int32 [65536], P('rows'), may hold values from 1 to 8
Outputs:
- centroids: bfloat16 [65536, 1024], P('rows')
- row_score: float32 [32768], P(('rows', 'rep'))
The draws below stay inside these ranges and needn't reach their ends.
Inputs may be any that keep to these rules, and one draw needn't show every extreme that they name: Within each device's aligned block of 1024 rows the assignments never fall. Cluster k belongs to owner k // 8192; in every block at most 256 rows belong to one owner, and some owner receives exactly 256 of them.
All inputs are finite; a program needn't handle non-finite values.
Results may differ from the reference program's by a relative error of at most 0.0028.
Values may be sent and summed in bfloat16 or wider, within the bound.
No kernel may reach another device: no remote copies, remote signals or barrier semaphores. Data moves between devices by JAX's collectives and lax.ppermute only.
A program may use at most 128 MiB of HBM per device.

```python
import jax
import jax.numpy as jnp
from jax import lax

D = 1024
CLUSTERS = 65536
ROW_DEV = 1024
OWNERS = 8
BLOCKS = 32
K_OWN = 8192
CAP = 256
ROWS_ALL = 32768


def draw_assign_block(key, hot_ids):
    k_one, k_two, k_three, k_four, k_five = jax.random.split(key, 5)
    half = CAP // 2
    spread = jax.random.randint(k_one, (OWNERS // 2,), 0, half + 1)
    spread = spread.at[0].set(half)
    load = jnp.concatenate([half + spread, half - spread])
    order = jax.random.permutation(k_two, OWNERS)
    loads = jnp.zeros((OWNERS,), jnp.int32).at[order].set(load.astype(jnp.int32))
    ends = jnp.cumsum(loads)
    position = jnp.arange(ROW_DEV, dtype=jnp.int32)
    owner_of = jnp.sum((position[:, None] >= ends[None, :]).astype(jnp.int32), axis=1)
    coin = jax.random.randint(k_three, (ROW_DEV,), 0, 2)
    pick = jax.random.randint(k_four, (ROW_DEV,), 0, 16)
    drawn = jax.random.randint(k_five, (ROW_DEV,), 0, K_OWN)
    hot_choice = hot_ids[owner_of, pick]
    local = jnp.where(coin == 1, hot_choice, drawn)
    return jnp.sort(owner_of * K_OWN + local).astype(jnp.int32)


def draw_assignments(key, part):
    hot_ids = jax.random.randint(jax.random.fold_in(key, 7), (OWNERS, 16), 0, K_OWN)
    keys = jax.random.split(jax.random.fold_in(key, 11), BLOCKS)
    blocks = jax.vmap(lambda one: draw_assign_block(one, hot_ids))(keys)
    return blocks.reshape(-1).astype(jnp.int32)


def place_ends(drawn, own_key, least, largest):
    longest = drawn.shape.index(max(drawn.shape))
    spots = []
    for shift in (0, 1):
        where = [jax.random.randint(jax.random.fold_in(own_key, axis), (), 0, length) for axis, length in enumerate(drawn.shape)]
        where[longest] = (where[longest] + shift) % drawn.shape[longest]
        spots.append(tuple(where))
    return drawn.at[spots[0]].set(least).at[spots[1]].set(largest)


def shard_levels(stream_key, shape, cuts, low, top_value):
    level, own = 1.0, jax.random.fold_in(stream_key, 6)
    for dim, parts in cuts:
        heights = jnp.exp(jax.random.uniform(jax.random.fold_in(own, dim), (parts,), jnp.float32, low / len(cuts), top_value / len(cuts)))
        level = level * jnp.repeat(heights, shape[dim] // parts).reshape([-1 if axis == dim else 1 for axis in range(len(shape))])
    return level


def centred(stream_key, shape, scale, limit, cuts=(), kind=jnp.bfloat16):
    array = jax.random.normal(stream_key, shape, jnp.float32) * scale
    if len(cuts) > 0:
        array = shard_levels(stream_key, shape, cuts, -0.22, 0.18) * array
    return jnp.clip(array, min=-limit, max=limit).astype(kind)


def setup_inputs(seed: int = 0) -> dict:
    splits = jax.random.split(jax.random.key(seed), 5)
    return {
        "embeddings": centred(splits[0], (ROWS_ALL, D), 0.03125, 0.25, ((0, 32),)),
        "assignments": draw_assignments(jax.random.fold_in(splits[4], 71), 0),
        "old_centroids": centred(splits[2], (CLUSTERS, D), 0.03125, 0.25, ((0, 8),)),
        "prior_counts": place_ends(jax.random.randint(splits[3], (CLUSTERS,), 1, 9), jax.random.fold_in(splits[3], 1), 1, 8).astype(jnp.int32),
    }


def reference(embeddings, assignments, old_centroids, prior_counts):
    values = embeddings.astype(jnp.float32)
    sums = jax.ops.segment_sum(values, assignments, num_segments=CLUSTERS)
    counts = jax.ops.segment_sum(jnp.ones(assignments.shape, jnp.float32), assignments, num_segments=CLUSTERS)
    prior = prior_counts.astype(jnp.float32)
    total = prior + counts
    mean = (prior[:, None] * old_centroids.astype(jnp.float32) + sums) / total[:, None]
    scale = lax.rsqrt(lax.optimization_barrier(jnp.sum(mean * mean, axis=1, keepdims=True)) + 1e-06)
    centroids = (mean * scale).astype(jnp.bfloat16)
    weight = (1.0 / total).astype(jnp.bfloat16)
    near = centroids[assignments].astype(jnp.float32)
    diff = values - near
    dist = lax.optimization_barrier(jnp.sum(diff * diff, axis=1))
    row_score = weight[assignments].astype(jnp.float32) * dist
    return (centroids, row_score)
```

```python
import jax
import jax.numpy as jnp
from jax import lax
from jax.experimental import pallas as pl
from jax.experimental.pallas import tpu as pltpu
from jax.sharding import PartitionSpec as P


LANES = 128
ROWS = 8
STEP = 8
DIGIT = 256


def chunk_sizes(cap):
    last = max(STEP, cap // 4 // STEP * STEP)
    first = max(STEP, cap * 3 // 8 // STEP * STEP)
    return [first, cap - first - last, last]


def pack_rows(starts, rows3, notes, owners, begins, sizes):
    tail = rows3.shape[1:]
    chunks = len(sizes)
    extra = [notes.shape[1] if notes is not None and c == 0 else 0 for c in range(chunks)]

    def body(starts_ref, rows_ref, *rest):
        if notes is not None:
            notes_ref, rest = rest[0], rest[1:]
        outs, sems = rest[:chunks], rest[chunks]

        def copies(owner):
            found = []
            for c in range(chunks):
                begin = starts_ref[owner] + begins[c]
                found.append((rows_ref.at[pl.ds(begin, sizes[c])], outs[c].at[owner, pl.ds(0, sizes[c])]))
            if notes is not None:
                found.append((notes_ref.at[owner], outs[0].at[owner, pl.ds(sizes[0], extra[0])]))
            return [
                pltpu.make_async_copy(source, target, sems.at[k, owner])
                for k, (source, target) in enumerate(found)
            ]

        def start(owner, _):
            for copy in copies(owner):
                copy.start()

        def wait(owner, _):
            for copy in copies(owner):
                copy.wait()

        lax.fori_loop(0, owners, start, None)
        lax.fori_loop(0, owners, wait, None)

    vmem = pl.BlockSpec(memory_space=pltpu.VMEM)
    return pl.pallas_call(
        body,
        in_specs=[pl.BlockSpec(memory_space=pltpu.SMEM), vmem] + [vmem] * (notes is not None),
        out_specs=[pl.BlockSpec(memory_space=pl.ANY)] * chunks,
        out_shape=[
            jax.ShapeDtypeStruct((owners, sizes[c] + extra[c]) + tail, rows3.dtype) for c in range(chunks)
        ],
        scratch_shapes=[pltpu.SemaphoreType.DMA((chunks + 1, owners))],
        name="pack_rows",
    )(starts, rows3, *([notes] if notes is not None else []))


def update(low, high, ids, prior, inverse, old, parts, owners, groups, sizes, pitches):
    clusters, width = old.shape
    chunks = len(parts)
    slabs = width // LANES
    subs = owners * groups
    tile = ROWS * LANES
    steps = clusters // tile
    trash = clusters * slabs
    offsets = [sum(sizes[:c]) for c in range(chunks)]

    def body(low_ref, high_ref, ids_ref, prior_ref, inverse_ref, old_ref, *rest):
        part_refs = rest[: chunks * groups]
        out_ref, dist_ref, acc = rest[chunks * groups : chunks * groups + 3]
        rows = rest[chunks * groups + 3 : chunks * groups + 3 + chunks]
        square, wide, norms, sems = rest[chunks * groups + 3 + chunks :]
        step = pl.program_id(0)

        def fetch(c, g):
            span = owners * pitches[c] * slabs
            return pltpu.make_async_copy(
                part_refs[c * groups + g], rows[c].at[pl.ds(g * span, span)], sems.at[c, g]
            )

        def picked(c, sub, at):
            base = offsets[c] * subs + sub * sizes[c] + at
            return [ids_ref[base + k] for k in range(STEP)]

        def load(c, sub, at):
            first = pl.multiple_of((sub * pitches[c] + at) * slabs, 2 * slabs)
            return rows[c][pl.ds(first, STEP * slabs), :].astype(jnp.float32)

        def spot(place):
            return pl.ds(place, slabs, stride=ROWS)

        def over_rows(c, sub, visit):
            lo = low_ref[c * subs + sub]
            hi = high_ref[c * subs + sub]
            lax.fori_loop(
                lo // STEP, (hi + STEP - 1) // STEP, lambda i, _: visit(i * STEP), None
            )

        def widen(ref):
            turned = ref[...].T
            for r in range(ROWS):
                wide[r * LANES : (r + 1) * LANES, :] = jnp.broadcast_to(
                    turned[:, r : r + 1], (LANES, LANES)
                )

        def place(first, at, half, j):
            return pl.ds(pl.multiple_of((first + at) * slabs + (half * slabs + j) * ROWS, ROWS), ROWS)

        @pl.when(step == 0)
        def _():
            for c in range(chunks):
                for g in range(groups):
                    fetch(c, g).start()

            def clear(i, _):
                where = pl.ds(pl.multiple_of(i * ROWS * LANES, ROWS * LANES), ROWS * LANES)
                acc[where, :] = jnp.zeros((ROWS * LANES, LANES), jnp.float32)

            lax.fori_loop(0, clusters * slabs // (ROWS * LANES), clear, None)
            acc[pl.ds(trash, ROWS * slabs), :] = jnp.zeros((ROWS * slabs, LANES), jnp.float32)
            for c in range(chunks):
                for g in range(groups):
                    fetch(c, g).wait()

                def add_sub(sub, _, c=c):
                    def add(at):
                        found = picked(c, sub, at)
                        new = load(c, sub, at)
                        was = [acc[spot(k), :] for k in found]
                        marks = [jnp.full((slabs, LANES), k, jnp.int32) for k in found]
                        now = []
                        for k in range(STEP):
                            base = was[k]
                            if k > 0:
                                base = jnp.where(marks[k] == marks[k - 1], now[-1], base)
                            now.append(base + new[k * slabs : (k + 1) * slabs])
                        for k in range(STEP):
                            acc[spot(found[k]), :] = now[k]

                    over_rows(c, sub, add)

                lax.fori_loop(0, subs, add_sub, None)

        first = step * tile
        widen(prior_ref)

        def measure(i, _):
            at = pl.multiple_of(i * 2 * ROWS, 2 * ROWS)
            weights = [wide[pl.ds(at + half * ROWS, ROWS), :] for half in range(2)]
            squares = [[], []]
            for j in range(slabs):
                before = old_ref[pl.ds(at, 2 * ROWS), j * LANES : (j + 1) * LANES].astype(jnp.float32)
                for half in range(2):
                    where = place(first, at, half, j)
                    value = weights[half] * before[half * ROWS : (half + 1) * ROWS] + acc[where, :]
                    acc[where, :] = value
                    squares[half].append(value * value)
            for half in range(2):
                parts = squares[half]
                while len(parts) > 1:
                    parts = [a + b for a, b in zip(parts[::2], parts[1::2])]
                norms[pl.ds(at + half * ROWS, ROWS), :] = parts[0]

        lax.fori_loop(0, tile // (2 * ROWS), measure, None, unroll=4)
        length = jnp.broadcast_to(jnp.sum(norms[...], axis=1, keepdims=True), (tile, LANES))
        widen(inverse_ref)
        factor = wide[...]
        wide[...] = factor * lax.rsqrt(factor * factor * length + 1e-06)

        def finish(i, _):
            at = pl.multiple_of(i * 2 * ROWS, 2 * ROWS)
            factors = [wide[pl.ds(at + half * ROWS, ROWS), :] for half in range(2)]
            for j in range(slabs):
                unit = jnp.concatenate(
                    [acc[place(first, at, half, j), :] * factors[half] for half in range(2)], axis=0
                ).astype(jnp.bfloat16)
                out_ref[pl.ds(at, 2 * ROWS), j * LANES : (j + 1) * LANES] = unit
                back = unit.astype(jnp.float32)
                for half in range(2):
                    acc[place(first, at, half, j), :] = back[half * ROWS : (half + 1) * ROWS]

        lax.fori_loop(0, tile // (2 * ROWS), finish, None, unroll=4)

        @pl.when(step == steps - 1)
        def _():
            for c in range(chunks):

                def score_sub(sub, _, c=c):
                    def score(at):
                        found = picked(c, sub, at)
                        new = load(c, sub, at)
                        for k in range(STEP):
                            gap = new[k * slabs : (k + 1) * slabs] - acc[spot(found[k]), :]
                            square[k * slabs : (k + 1) * slabs, :] = gap * gap
                        total = square[pl.ds(0, STEP, stride=slabs), :]
                        for j in range(1, slabs):
                            total = total + square[pl.ds(j, STEP, stride=slabs), :]
                        where = pl.multiple_of(offsets[c] * owners + sub * sizes[c] + at, STEP)
                        dist_ref[pl.ds(where, STEP), :] = total

                    over_rows(c, sub, score)

                lax.fori_loop(0, owners, score_sub, None)

    smem = pl.BlockSpec(memory_space=pltpu.SMEM)
    own = owners * sum(sizes)
    here = lambda i: (i, 0)
    return pl.pallas_call(
        body,
        grid=(steps,),
        in_specs=[
            smem,
            smem,
            smem,
            pl.BlockSpec((ROWS, LANES), here),
            pl.BlockSpec((ROWS, LANES), here),
            pl.BlockSpec((tile, width), here),
        ]
        + [pl.BlockSpec(memory_space=pl.ANY)] * (chunks * groups),
        out_specs=[pl.BlockSpec((tile, width), here), pl.BlockSpec((own, LANES), lambda i: (0, 0))],
        out_shape=[
            jax.ShapeDtypeStruct((clusters, width), jnp.bfloat16),
            jax.ShapeDtypeStruct((own, LANES), jnp.float32),
        ],
        scratch_shapes=[pltpu.VMEM(((clusters + ROWS) * slabs, LANES), jnp.float32)]
        + [pltpu.VMEM((subs * pitch * slabs, LANES), jnp.bfloat16) for pitch in pitches]
        + [
            pltpu.VMEM((STEP * slabs, LANES), jnp.float32),
            pltpu.VMEM((tile, LANES), jnp.float32),
            pltpu.VMEM((tile, LANES), jnp.float32),
            pltpu.SemaphoreType.DMA((chunks, groups)),
        ],
        compiler_params=pltpu.CompilerParams(
            dimension_semantics=("arbitrary",), vmem_limit_bytes=61 * 1024 * 1024
        ),
        name="update_centroids",
    )(low, high, ids, prior, inverse, old, *[piece for part in parts for piece in part])


def two_level(rel, clusters):
    high = (rel // LANES)[:, None] == jnp.arange(clusters // LANES, dtype=jnp.int32)[None, :]
    low = (rel % LANES)[:, None] == jnp.arange(LANES, dtype=jnp.int32)[None, :]
    return high.astype(jnp.bfloat16), low


def spread(own, groups):
    pieces, hop = [own], groups // 2
    while hop > 0:
        pairs = [(source, source ^ hop) for source in range(groups)]
        more = []
        for piece in pieces:
            more.append(lax.ppermute(piece, "rep", pairs))
        pieces = pieces + more
        hop //= 2
    return pieces


def write_notes(rel, clusters, width, slabs):
    owners, cap = rel.shape
    upper = jnp.where(rel < 0, -1, jnp.where(rel < clusters, rel // DIGIT, DIGIT))
    lower = jnp.where((rel >= 0) & (rel < clusters), rel % DIGIT, 0)
    count = -(-cap // width)
    digits = [
        jnp.pad(part, ((0, 0), (0, count * width - cap))).reshape(owners, count, slabs, LANES)
        for part in (upper, lower)
    ]
    return jnp.concatenate(digits, axis=1).astype(jnp.bfloat16)


def read_notes(notes, cap):
    owners, _ = notes.shape[:2]
    digits = notes.astype(jnp.int32).reshape(owners, 2, -1)[:, :, :cap]
    return digits[:, 0] * DIGIT + digits[:, 1]


def on_device(embeddings, assignments, old_centroids, prior_counts):
    rows_here, width = embeddings.shape
    owners = lax.axis_size("rows")
    groups = lax.axis_size("rep")
    clusters = old_centroids.shape[0]
    assert clusters < DIGIT * DIGIT and groups & (groups - 1) == 0
    cap = 2 * rows_here // owners
    sizes = chunk_sizes(cap)
    chunks = len(sizes)
    begins = [sum(sizes[:c]) for c in range(chunks)]
    slabs = width // LANES

    owner = jnp.arange(owners, dtype=jnp.int32)
    bounds = owner * clusters
    starts = jnp.sum((assignments[None, :] < bounds[:, None]).astype(jnp.int32), axis=1)
    starts = jnp.minimum(starts, rows_here - cap)
    slot_row = (starts[:, None] + jnp.arange(cap, dtype=jnp.int32)[None, :]).reshape(-1)
    row = jnp.arange(rows_here, dtype=jnp.int32)
    slot_ids = jnp.sum(
        jnp.where(slot_row[:, None] == row[None, :], assignments[None, :], 0), axis=1
    ).reshape(owners, cap)
    notes = write_notes(slot_ids - bounds[:, None], clusters, width, slabs)

    rows3 = embeddings.reshape(rows_here, slabs, LANES)
    packed = list(pack_rows(starts, rows3, notes, owners, begins[:1], sizes[:1]))
    packed += list(pack_rows(starts, rows3, None, owners, begins[1:], sizes[1:]))
    pitches = [pack.shape[1] for pack in packed]

    parts = []
    for c in range(chunks):
        came = lax.all_to_all(packed[c], "rows", split_axis=0, concat_axis=0, tiled=True)
        pieces = spread(came, groups)
        if c == 0:
            every = [read_notes(piece[:, sizes[0] :], cap) for piece in pieces]
        parts.append([piece.reshape(owners * pitches[c] * slabs, LANES) for piece in pieces])
    rel = jnp.concatenate(every, axis=0)

    inside = (rel >= 0) & (rel < clusters)
    spots = jnp.where(inside, rel, clusters)
    spots = spots // ROWS * (ROWS * slabs) + spots % ROWS
    split = [rel[:, begins[c] : begins[c] + sizes[c]] for c in range(chunks)]
    spots = jnp.concatenate(
        [spots[:, begins[c] : begins[c] + sizes[c]].reshape(-1) for c in range(chunks)]
    )
    low = jnp.concatenate([jnp.sum((part < 0).astype(jnp.int32), axis=1) for part in split])
    high = jnp.concatenate([jnp.sum((part < clusters).astype(jnp.int32), axis=1) for part in split])

    flat = rel.reshape(-1)
    live = (flat >= 0) & (flat < clusters)
    hot_high, hot_low = two_level(jnp.where(live, flat, -1), clusters)
    counts = lax.dot_general(
        hot_high,
        (hot_low & live[:, None]).astype(jnp.bfloat16),
        (((0,), (0,)), ((), ())),
        preferred_element_type=jnp.float32,
    )
    prior = prior_counts.astype(jnp.float32).reshape(clusters // LANES, LANES)
    inverse = 1.0 / (prior + counts)

    centroids, partial = update(
        low, high, spots, prior, inverse, old_centroids, parts, owners, groups, sizes, pitches
    )

    mine = every[0].reshape(-1)
    mine_live = (mine >= 0) & (mine < clusters)
    my_high, my_low = two_level(jnp.where(mine_live, mine, 0), clusters)
    lanes = lax.dot_general(
        my_high,
        inverse.astype(jnp.bfloat16),
        (((1,), (0,)), ((), ())),
        preferred_element_type=jnp.float32,
    )
    my_weight = jnp.sum(jnp.where(my_low, lanes, 0.0), axis=1)

    dist = jnp.sum(partial, axis=1)
    dist = jnp.concatenate(
        [
            dist[owners * begins[c] : owners * (begins[c] + sizes[c])].reshape(owners, sizes[c])
            for c in range(chunks)
        ],
        axis=1,
    ).reshape(-1)
    scores = jnp.where(mine_live, my_weight * dist, 0.0).reshape(owners, cap)
    got = lax.all_to_all(scores, "rows", split_axis=0, concat_axis=0, tiled=True).reshape(-1)
    row_owner = assignments // clusters
    slot_owner = jnp.repeat(owner, cap)
    match = (slot_row[None, :] == row[:, None]) & (slot_owner[None, :] == row_owner[:, None])
    row_score = jnp.sum(jnp.where(match, got[None, :], 0.0), axis=1)
    return (centroids, row_score)


def solution(mesh):
    placed = (P(("rows", "rep"), None), P(("rows", "rep")), P("rows", None), P("rows"))
    return jax.shard_map(
        on_device,
        mesh=mesh,
        in_specs=placed,
        out_specs=(P("rows", None), P(("rows", "rep"))),
        check_vma=False,
    )
```

```python
import jax
import jax.numpy as jnp
from jax import lax
from jax.experimental import pallas as pl
from jax.experimental.pallas import tpu as pltpu
from jax.sharding import PartitionSpec as P


LANES = 128
ROWS = 8
STEP = 8
PAIR = 2
DIGIT = 256


CHUNKS = 4


def chunk_sizes(cap):
    less = cap // 16 // STEP * STEP
    last = (cap // CHUNKS - less * (CHUNKS - 1) // 2) // STEP * STEP
    sizes = [last + less * (CHUNKS - 1 - c) for c in range(CHUNKS)]
    return [sizes[0] + cap - sum(sizes)] + sizes[1:]


def pack_rows(starts, rows3, notes, owners, begins, sizes):
    tail = rows3.shape[1:]
    chunks = len(sizes)
    extra = [notes.shape[1] if notes is not None and c == 0 else 0 for c in range(chunks)]

    def body(starts_ref, rows_ref, *rest):
        if notes is not None:
            notes_ref, rest = rest[0], rest[1:]
        outs, sems = rest[:chunks], rest[chunks]

        def copies(owner):
            found = []
            for c in range(chunks):
                begin = starts_ref[owner] + begins[c]
                found.append((rows_ref.at[pl.ds(begin, sizes[c])], outs[c].at[owner, pl.ds(0, sizes[c])]))
            if notes is not None:
                found.append((notes_ref.at[owner], outs[0].at[owner, pl.ds(sizes[0], extra[0])]))
            return [
                pltpu.make_async_copy(source, target, sems.at[k, owner])
                for k, (source, target) in enumerate(found)
            ]

        def start(owner, _):
            for copy in copies(owner):
                copy.start()

        def wait(owner, _):
            for copy in copies(owner):
                copy.wait()

        lax.fori_loop(0, owners, start, None)
        lax.fori_loop(0, owners, wait, None)

    vmem = pl.BlockSpec(memory_space=pltpu.VMEM)
    return pl.pallas_call(
        body,
        in_specs=[pl.BlockSpec(memory_space=pltpu.SMEM), vmem] + [vmem] * (notes is not None),
        out_specs=[pl.BlockSpec(memory_space=pl.ANY)] * chunks,
        out_shape=[
            jax.ShapeDtypeStruct((owners, sizes[c] + extra[c]) + tail, rows3.dtype) for c in range(chunks)
        ],
        scratch_shapes=[pltpu.SemaphoreType.DMA((chunks + 1, owners))],
        name="pack_rows",
    )(starts, rows3, *([notes] if notes is not None else []))


def update(low, high, ids, prior, inverse, old, parts, owners, groups, sizes, pitches):
    clusters, width = old.shape
    chunks = len(parts)
    slabs = width // LANES
    subs = owners * groups
    tile = ROWS * LANES
    steps = clusters // tile
    trash = clusters * slabs
    offsets = [sum(sizes[:c]) for c in range(chunks)]

    def body(low_ref, high_ref, ids_ref, prior_ref, inverse_ref, old_ref, *rest):
        part_refs = rest[: chunks * groups]
        out_ref, dist_ref, acc = rest[chunks * groups : chunks * groups + 3]
        rows = rest[chunks * groups + 3 : chunks * groups + 3 + chunks]
        square, wide, norms, sems = rest[chunks * groups + 3 + chunks :]
        step = pl.program_id(0)

        def fetch(c, g):
            span = owners * pitches[c] * slabs
            return pltpu.make_async_copy(
                part_refs[c * groups + g], rows[c].at[pl.ds(g * span, span)], sems.at[c, g]
            )

        def picked(c, sub, at):
            base = offsets[c] * subs + sub * sizes[c] + at
            return [ids_ref[base + k] for k in range(STEP)]

        def load(c, sub, at):
            first = pl.multiple_of((sub * pitches[c] + at) * slabs, 2 * slabs)
            return rows[c][pl.ds(first, STEP * slabs), :].astype(jnp.float32)

        def spot(place):
            return pl.ds(place, slabs, stride=ROWS)

        def over_rows(c, sub, visit):
            lo = low_ref[c * subs + sub]
            hi = high_ref[c * subs + sub]
            lax.fori_loop(
                lo // STEP, (hi + STEP - 1) // STEP, lambda i, _: visit(i * STEP), None
            )

        def widen(ref):
            turned = ref[...].T
            for r in range(ROWS):
                wide[r * LANES : (r + 1) * LANES, :] = jnp.broadcast_to(
                    turned[:, r : r + 1], (LANES, LANES)
                )

        def place(first, at, half, j):
            return pl.ds(pl.multiple_of((first + at) * slabs + (half * slabs + j) * ROWS, ROWS), ROWS)

        @pl.when(step == 0)
        def _():
            for c in range(chunks):
                for g in range(groups):
                    fetch(c, g).start()

            def clear(i, _):
                where = pl.ds(pl.multiple_of(i * ROWS * LANES, ROWS * LANES), ROWS * LANES)
                acc[where, :] = jnp.zeros((ROWS * LANES, LANES), jnp.float32)

            lax.fori_loop(0, clusters * slabs // (ROWS * LANES), clear, None)
            acc[pl.ds(trash, ROWS * slabs), :] = jnp.zeros((ROWS * slabs, LANES), jnp.float32)
            for c in range(chunks):
                for g in range(groups):
                    fetch(c, g).wait()

                def add_sub(sub, _, c=c):
                    def add(at):
                        found = picked(c, sub, at)
                        new = load(c, sub, at)
                        was = [acc[spot(k), :] for k in found]
                        marks = [jnp.full((slabs, LANES), k, jnp.int32) for k in found]
                        now = []
                        for k in range(STEP):
                            base = was[k]
                            if k > 0:
                                base = jnp.where(marks[k] == marks[k - 1], now[-1], base)
                            now.append(base + new[k * slabs : (k + 1) * slabs])
                        for k in range(STEP):
                            acc[spot(found[k]), :] = now[k]

                    over_rows(c, sub, add)

                lax.fori_loop(0, subs, add_sub, None)

        first = step * tile
        widen(prior_ref)

        def measure(i, _):
            at = pl.multiple_of(i * 2 * ROWS, 2 * ROWS)
            weights = [wide[pl.ds(at + half * ROWS, ROWS), :] for half in range(2)]
            squares = [[], []]
            for j in range(slabs):
                before = old_ref[pl.ds(at, 2 * ROWS), j * LANES : (j + 1) * LANES].astype(jnp.float32)
                for half in range(2):
                    where = place(first, at, half, j)
                    value = weights[half] * before[half * ROWS : (half + 1) * ROWS] + acc[where, :]
                    acc[where, :] = value
                    squares[half].append(value * value)
            for half in range(2):
                parts = squares[half]
                while len(parts) > 1:
                    parts = [a + b for a, b in zip(parts[::2], parts[1::2])]
                norms[pl.ds(at + half * ROWS, ROWS), :] = parts[0]

        lax.fori_loop(0, tile // (2 * ROWS), measure, None, unroll=4)
        length = jnp.broadcast_to(jnp.sum(norms[...], axis=1, keepdims=True), (tile, LANES))
        widen(inverse_ref)
        factor = wide[...]
        wide[...] = factor * lax.rsqrt(factor * factor * length + 1e-06)

        def finish(i, _):
            at = pl.multiple_of(i * 2 * ROWS, 2 * ROWS)
            factors = [wide[pl.ds(at + half * ROWS, ROWS), :] for half in range(2)]
            for j in range(slabs):
                unit = jnp.concatenate(
                    [acc[place(first, at, half, j), :] * factors[half] for half in range(2)], axis=0
                ).astype(jnp.bfloat16)
                out_ref[pl.ds(at, 2 * ROWS), j * LANES : (j + 1) * LANES] = unit
                back = unit.astype(jnp.float32)
                for half in range(2):
                    acc[place(first, at, half, j), :] = back[half * ROWS : (half + 1) * ROWS]

        lax.fori_loop(0, tile // (2 * ROWS), finish, None, unroll=4)

        @pl.when(step == steps - 1)
        def _():
            for c in range(chunks):

                def score_sub(sub, _, c=c):
                    begin = low_ref[c * subs + sub] // STEP
                    end = (high_ref[c * subs + sub] + STEP - 1) // STEP

                    def score(i, _):
                        for lane in range(PAIR):
                            at = jnp.minimum(begin + i * PAIR + lane, end - 1) * STEP
                            found = picked(c, sub, at)
                            new = load(c, sub, at)
                            gaps = [
                                new[k * slabs : (k + 1) * slabs] - acc[spot(found[k]), :]
                                for k in range(STEP)
                            ]
                            for k in range(STEP):
                                square[lane, k * slabs : (k + 1) * slabs, :] = gaps[k] * gaps[k]
                        for lane in range(PAIR):
                            at = jnp.minimum(begin + i * PAIR + lane, end - 1) * STEP
                            terms = [square[lane, pl.ds(j, STEP, stride=slabs), :] for j in range(slabs)]
                            while len(terms) > 1:
                                terms = [a + b for a, b in zip(terms[::2], terms[1::2])]
                            where = pl.multiple_of(offsets[c] * owners + sub * sizes[c] + at, STEP)
                            dist_ref[pl.ds(where, STEP), :] = terms[0]

                    lax.fori_loop(0, (end - begin + PAIR - 1) // PAIR, score, None)

                lax.fori_loop(0, owners, score_sub, None)

    smem = pl.BlockSpec(memory_space=pltpu.SMEM)
    own = owners * sum(sizes)
    here = lambda i: (i, 0)
    return pl.pallas_call(
        body,
        grid=(steps,),
        in_specs=[
            smem,
            smem,
            smem,
            pl.BlockSpec((ROWS, LANES), here),
            pl.BlockSpec((ROWS, LANES), here),
            pl.BlockSpec((tile, width), here),
        ]
        + [pl.BlockSpec(memory_space=pltpu.HBM)] * (chunks * groups),
        out_specs=[pl.BlockSpec((tile, width), here), pl.BlockSpec((own, LANES), lambda i: (0, 0))],
        out_shape=[
            jax.ShapeDtypeStruct((clusters, width), jnp.bfloat16),
            jax.ShapeDtypeStruct((own, LANES), jnp.float32),
        ],
        scratch_shapes=[pltpu.VMEM(((clusters + ROWS) * slabs, LANES), jnp.float32)]
        + [pltpu.VMEM((subs * pitch * slabs, LANES), jnp.bfloat16) for pitch in pitches]
        + [
            pltpu.VMEM((PAIR, STEP * slabs, LANES), jnp.float32),
            pltpu.VMEM((tile, LANES), jnp.float32),
            pltpu.VMEM((tile, LANES), jnp.float32),
            pltpu.SemaphoreType.DMA((chunks, groups)),
        ],
        compiler_params=pltpu.CompilerParams(
            dimension_semantics=("arbitrary",), vmem_limit_bytes=61 * 1024 * 1024
        ),
        name="update_centroids",
    )(low, high, ids, prior, inverse, old, *[piece for part in parts for piece in part])


def two_level(rel, clusters):
    high = (rel // LANES)[:, None] == jnp.arange(clusters // LANES, dtype=jnp.int32)[None, :]
    low = (rel % LANES)[:, None] == jnp.arange(LANES, dtype=jnp.int32)[None, :]
    return high.astype(jnp.bfloat16), low


def spread(own, groups):
    pieces, hop = [own], groups // 2
    while hop > 0:
        pairs = [(source, source ^ hop) for source in range(groups)]
        more = []
        for piece in pieces:
            more.append(lax.ppermute(piece, "rep", pairs))
        pieces = pieces + more
        hop //= 2
    return pieces


def write_notes(rel, clusters, width, slabs):
    owners, cap = rel.shape
    upper = jnp.where(rel < 0, -1, jnp.where(rel < clusters, rel // DIGIT, DIGIT))
    lower = jnp.where((rel >= 0) & (rel < clusters), rel % DIGIT, 0)
    count = -(-cap // width)
    digits = [
        jnp.pad(part, ((0, 0), (0, count * width - cap))).reshape(owners, count, slabs, LANES)
        for part in (upper, lower)
    ]
    return jnp.concatenate(digits, axis=1).astype(jnp.bfloat16)


def read_notes(notes, cap):
    owners, _ = notes.shape[:2]
    digits = notes.astype(jnp.int32).reshape(owners, 2, -1)[:, :, :cap]
    return digits[:, 0] * DIGIT + digits[:, 1]


def on_device(embeddings, assignments, old_centroids, prior_counts):
    rows_here, width = embeddings.shape
    owners = lax.axis_size("rows")
    groups = lax.axis_size("rep")
    clusters = old_centroids.shape[0]
    assert clusters < DIGIT * DIGIT and groups & (groups - 1) == 0
    cap = 2 * rows_here // owners
    sizes = chunk_sizes(cap)
    chunks = len(sizes)
    begins = [sum(sizes[:c]) for c in range(chunks)]
    slabs = width // LANES

    owner = jnp.arange(owners, dtype=jnp.int32)
    bounds = owner * clusters
    starts = jnp.sum((assignments[None, :] < bounds[:, None]).astype(jnp.int32), axis=1)
    starts = jnp.minimum(starts, rows_here - cap)
    slot_row = (starts[:, None] + jnp.arange(cap, dtype=jnp.int32)[None, :]).reshape(-1)
    row = jnp.arange(rows_here, dtype=jnp.int32)
    slot_ids = jnp.sum(
        jnp.where(slot_row[:, None] == row[None, :], assignments[None, :], 0), axis=1
    ).reshape(owners, cap)
    notes = write_notes(slot_ids - bounds[:, None], clusters, width, slabs)

    rows3 = embeddings.reshape(rows_here, slabs, LANES)
    packed = list(pack_rows(starts, rows3, None, owners, begins[:1], sizes[:1]))
    packed += list(pack_rows(starts, rows3, notes, owners, begins[1:], sizes[1:]))
    pitches = [pack.shape[1] for pack in packed]

    parts = []
    for c in range(chunks):
        came = lax.all_to_all(packed[c], "rows", split_axis=0, concat_axis=0, tiled=True)
        pieces = spread(came, groups)
        if c == 1:
            noted = [piece[:, sizes[1] :] for piece in pieces]
        parts.append([piece.reshape(owners * pitches[c] * slabs, LANES) for piece in pieces])
    every = [read_notes(piece, cap) for piece in noted]
    rel = jnp.concatenate(every, axis=0)

    inside = (rel >= 0) & (rel < clusters)
    spots = jnp.where(inside, rel, clusters)
    spots = spots // ROWS * (ROWS * slabs) + spots % ROWS
    split = [rel[:, begins[c] : begins[c] + sizes[c]] for c in range(chunks)]
    spots = jnp.concatenate(
        [spots[:, begins[c] : begins[c] + sizes[c]].reshape(-1) for c in range(chunks)]
    )
    low = jnp.concatenate([jnp.sum((part < 0).astype(jnp.int32), axis=1) for part in split])
    high = jnp.concatenate([jnp.sum((part < clusters).astype(jnp.int32), axis=1) for part in split])

    flat = rel.reshape(-1)
    live = (flat >= 0) & (flat < clusters)
    hot_high, hot_low = two_level(jnp.where(live, flat, -1), clusters)
    counts = lax.dot_general(
        hot_high,
        (hot_low & live[:, None]).astype(jnp.bfloat16),
        (((0,), (0,)), ((), ())),
        preferred_element_type=jnp.float32,
    )
    prior = prior_counts.astype(jnp.float32).reshape(clusters // LANES, LANES)
    inverse = 1.0 / (prior + counts)

    mine = every[0].reshape(-1)
    mine_live = (mine >= 0) & (mine < clusters)
    my_high, my_low = two_level(jnp.where(mine_live, mine, 0), clusters)
    lanes = lax.dot_general(
        my_high,
        inverse.astype(jnp.bfloat16),
        (((1,), (0,)), ((), ())),
        preferred_element_type=jnp.float32,
    )
    my_weight = jnp.sum(jnp.where(my_low, lanes, 0.0), axis=1)

    centroids, partial = update(
        low, high, spots, prior, inverse, old_centroids, parts, owners, groups, sizes, pitches
    )

    dist = jnp.sum(partial, axis=1)
    dist = jnp.concatenate(
        [
            dist[owners * begins[c] : owners * (begins[c] + sizes[c])].reshape(owners, sizes[c])
            for c in range(chunks)
        ],
        axis=1,
    ).reshape(-1)
    scores = jnp.where(mine_live, my_weight * dist, 0.0).reshape(owners, cap)
    got = lax.all_to_all(scores, "rows", split_axis=0, concat_axis=0, tiled=True).reshape(-1)
    row_owner = assignments // clusters
    slot_owner = jnp.repeat(owner, cap)
    match = (slot_row[None, :] == row[:, None]) & (slot_owner[None, :] == row_owner[:, None])
    row_score = jnp.sum(jnp.where(match, got[None, :], 0.0), axis=1)
    return (centroids, row_score)


def solution(mesh):
    placed = (P(("rows", "rep"), None), P(("rows", "rep")), P("rows", None), P("rows"))
    return jax.shard_map(
        on_device,
        mesh=mesh,
        in_specs=placed,
        out_specs=(P("rows", None), P(("rows", "rep"))),
        check_vma=False,
    )
```

```python
import jax
import jax.numpy as jnp
from jax import lax
from jax.experimental import pallas as pl
from jax.experimental.pallas import tpu as pltpu
from jax.sharding import PartitionSpec as P


LANES = 128
ROWS = 8
STEP = 8
PAIR = 2
DIGIT = 256


CHUNKS = 4


def chunk_sizes(cap):
    less = cap // 16 // STEP * STEP
    last = (cap // CHUNKS - less * (CHUNKS - 1) // 2) // STEP * STEP
    sizes = [last + less * (CHUNKS - 1 - c) for c in range(CHUNKS)]
    return [sizes[0] + cap - sum(sizes)] + sizes[1:]


def pack_rows(starts, rows3, notes, owners, begins, sizes):
    tail = rows3.shape[1:]
    chunks = len(sizes)
    extra = [notes.shape[1] if notes is not None and c == 0 else 0 for c in range(chunks)]

    def body(starts_ref, rows_ref, *rest):
        if notes is not None:
            notes_ref, rest = rest[0], rest[1:]
        outs, sems = rest[:chunks], rest[chunks]

        def copies(owner):
            found = []
            for c in range(chunks):
                begin = starts_ref[owner] + begins[c]
                found.append((rows_ref.at[pl.ds(begin, sizes[c])], outs[c].at[owner, pl.ds(0, sizes[c])]))
            if notes is not None:
                found.append((notes_ref.at[owner], outs[0].at[owner, pl.ds(sizes[0], extra[0])]))
            return [
                pltpu.make_async_copy(source, target, sems.at[k, owner])
                for k, (source, target) in enumerate(found)
            ]

        def start(owner, _):
            for copy in copies(owner):
                copy.start()

        def wait(owner, _):
            for copy in copies(owner):
                copy.wait()

        lax.fori_loop(0, owners, start, None)
        lax.fori_loop(0, owners, wait, None)

    vmem = pl.BlockSpec(memory_space=pltpu.VMEM)
    return pl.pallas_call(
        body,
        in_specs=[pl.BlockSpec(memory_space=pltpu.SMEM), vmem] + [vmem] * (notes is not None),
        out_specs=[pl.BlockSpec(memory_space=pl.ANY)] * chunks,
        out_shape=[
            jax.ShapeDtypeStruct((owners, sizes[c] + extra[c]) + tail, rows3.dtype) for c in range(chunks)
        ],
        scratch_shapes=[pltpu.SemaphoreType.DMA((chunks + 1, owners))],
        name="pack_rows",
    )(starts, rows3, *([notes] if notes is not None else []))


def update(low, high, ids, prior, inverse, old, parts, owners, groups, sizes, pitches):
    clusters, width = old.shape
    chunks = len(parts)
    slabs = width // LANES
    subs = owners * groups
    tile = ROWS * LANES
    steps = clusters // tile
    trash = clusters * slabs
    offsets = [sum(sizes[:c]) for c in range(chunks)]

    def body(low_ref, high_ref, ids_ref, prior_ref, inverse_ref, old_ref, *rest):
        part_refs = rest[: chunks * groups]
        out_ref, dist_ref, acc = rest[chunks * groups : chunks * groups + 3]
        rows = rest[chunks * groups + 3 : chunks * groups + 3 + chunks]
        square, wide, norms, scales, sems = rest[chunks * groups + 3 + chunks :]
        step = pl.program_id(0)

        def fetch(c, g):
            span = owners * pitches[c] * slabs
            return pltpu.make_async_copy(
                part_refs[c * groups + g], rows[c].at[pl.ds(g * span, span)], sems.at[c, g]
            )

        def picked(c, sub, at):
            base = offsets[c] * subs + sub * sizes[c] + at
            return [ids_ref[base + k] for k in range(STEP)]

        def load(c, sub, at):
            first = pl.multiple_of((sub * pitches[c] + at) * slabs, 2 * slabs)
            return rows[c][pl.ds(first, STEP * slabs), :].astype(jnp.float32)

        def cluster_of(place):
            shift = (ROWS * slabs).bit_length() - 1
            return (place >> shift) * ROWS + (place & (ROWS - 1))

        def spot(place):
            return pl.ds(place, slabs, stride=ROWS)

        def over_rows(c, sub, visit):
            lo = low_ref[c * subs + sub]
            hi = high_ref[c * subs + sub]
            lax.fori_loop(
                lo // STEP, (hi + STEP - 1) // STEP, lambda i, _: visit(i * STEP), None
            )

        def widen(ref):
            turned = ref[...].T
            for r in range(ROWS):
                wide[r * LANES : (r + 1) * LANES, :] = jnp.broadcast_to(
                    turned[:, r : r + 1], (LANES, LANES)
                )

        def place(first, at, half, j):
            return pl.ds(pl.multiple_of((first + at) * slabs + (half * slabs + j) * ROWS, ROWS), ROWS)

        @pl.when(step == 0)
        def _():
            for c in range(chunks):
                for g in range(groups):
                    fetch(c, g).start()

            def clear(i, _):
                where = pl.ds(pl.multiple_of(i * ROWS * LANES, ROWS * LANES), ROWS * LANES)
                acc[where, :] = jnp.zeros((ROWS * LANES, LANES), jnp.float32)

            lax.fori_loop(0, clusters * slabs // (ROWS * LANES), clear, None)
            acc[pl.ds(trash, ROWS * slabs), :] = jnp.zeros((ROWS * slabs, LANES), jnp.float32)
            for c in range(chunks):
                for g in range(groups):
                    fetch(c, g).wait()

                def add_sub(sub, _, c=c):
                    def add(at):
                        found = picked(c, sub, at)
                        new = load(c, sub, at)
                        was = [acc[spot(k), :] for k in found]
                        marks = [jnp.full((slabs, LANES), k, jnp.int32) for k in found]
                        now = []
                        for k in range(STEP):
                            base = was[k]
                            if k > 0:
                                base = jnp.where(marks[k] == marks[k - 1], now[-1], base)
                            now.append(base + new[k * slabs : (k + 1) * slabs])
                        for k in range(STEP):
                            acc[spot(found[k]), :] = now[k]

                    over_rows(c, sub, add)

                lax.fori_loop(0, subs, add_sub, None)

        first = step * tile
        widen(prior_ref)

        def measure(i, _):
            at = pl.multiple_of(i * 2 * ROWS, 2 * ROWS)
            weights = [wide[pl.ds(at + half * ROWS, ROWS), :] for half in range(2)]
            squares = [[], []]
            for j in range(slabs):
                before = old_ref[pl.ds(at, 2 * ROWS), j * LANES : (j + 1) * LANES].astype(jnp.float32)
                for half in range(2):
                    where = place(first, at, half, j)
                    value = weights[half] * before[half * ROWS : (half + 1) * ROWS] + acc[where, :]
                    acc[where, :] = value
                    squares[half].append(value * value)
            for half in range(2):
                parts = squares[half]
                while len(parts) > 1:
                    parts = [a + b for a, b in zip(parts[::2], parts[1::2])]
                norms[pl.ds(at + half * ROWS, ROWS), :] = parts[0]

        lax.fori_loop(0, tile // (2 * ROWS), measure, None, unroll=4)
        length = jnp.broadcast_to(jnp.sum(norms[...], axis=1, keepdims=True), (tile, LANES))
        widen(inverse_ref)
        factor = wide[...]
        scales[pl.ds(pl.multiple_of(first, tile), tile), :] = factor * lax.rsqrt(
            factor * factor * length + 1e-06
        )

        def finish(i, _):
            at = pl.multiple_of(i * 2 * ROWS, 2 * ROWS)
            factors = [scales[pl.ds(first + at + half * ROWS, ROWS), :] for half in range(2)]
            for j in range(slabs):
                unit = jnp.concatenate(
                    [acc[place(first, at, half, j), :] * factors[half] for half in range(2)], axis=0
                ).astype(jnp.bfloat16)
                out_ref[pl.ds(at, 2 * ROWS), j * LANES : (j + 1) * LANES] = unit

        lax.fori_loop(0, tile // (2 * ROWS), finish, None, unroll=4)

        @pl.when(step == steps - 1)
        def _():
            for c in range(chunks):

                def score_sub(sub, _, c=c):
                    begin = low_ref[c * subs + sub] // STEP
                    end = (high_ref[c * subs + sub] + STEP - 1) // STEP

                    def score(i, _):
                        for lane in range(PAIR):
                            at = jnp.minimum(begin + i * PAIR + lane, end - 1) * STEP
                            found = picked(c, sub, at)
                            new = load(c, sub, at)
                            near = [
                                (acc[spot(k), :] * scales[pl.ds(cluster_of(k), 1), :])
                                .astype(jnp.bfloat16)
                                .astype(jnp.float32)
                                for k in found
                            ]
                            gaps = [new[k * slabs : (k + 1) * slabs] - near[k] for k in range(STEP)]
                            for k in range(STEP):
                                square[lane, k * slabs : (k + 1) * slabs, :] = gaps[k] * gaps[k]
                        for lane in range(PAIR):
                            at = jnp.minimum(begin + i * PAIR + lane, end - 1) * STEP
                            terms = [square[lane, pl.ds(j, STEP, stride=slabs), :] for j in range(slabs)]
                            while len(terms) > 1:
                                terms = [a + b for a, b in zip(terms[::2], terms[1::2])]
                            where = pl.multiple_of(offsets[c] * owners + sub * sizes[c] + at, STEP)
                            dist_ref[pl.ds(where, STEP), :] = terms[0]

                    lax.fori_loop(0, (end - begin + PAIR - 1) // PAIR, score, None)

                lax.fori_loop(0, owners, score_sub, None)

    smem = pl.BlockSpec(memory_space=pltpu.SMEM)
    own = owners * sum(sizes)
    here = lambda i: (i, 0)
    return pl.pallas_call(
        body,
        grid=(steps,),
        in_specs=[
            smem,
            smem,
            smem,
            pl.BlockSpec((ROWS, LANES), here),
            pl.BlockSpec((ROWS, LANES), here),
            pl.BlockSpec((tile, width), here),
        ]
        + [pl.BlockSpec(memory_space=pltpu.HBM)] * (chunks * groups),
        out_specs=[pl.BlockSpec((tile, width), here), pl.BlockSpec((own, LANES), lambda i: (0, 0), pipeline_mode=pl.Buffered(1))],
        out_shape=[
            jax.ShapeDtypeStruct((clusters, width), jnp.bfloat16),
            jax.ShapeDtypeStruct((own, LANES), jnp.float32),
        ],
        scratch_shapes=[pltpu.VMEM(((clusters + ROWS) * slabs, LANES), jnp.float32)]
        + [pltpu.VMEM((subs * pitch * slabs, LANES), jnp.bfloat16) for pitch in pitches]
        + [
            pltpu.VMEM((PAIR, STEP * slabs, LANES), jnp.float32),
            pltpu.VMEM((tile, LANES), jnp.float32),
            pltpu.VMEM((tile, LANES), jnp.float32),
            pltpu.VMEM((clusters + ROWS, LANES), jnp.float32),
            pltpu.SemaphoreType.DMA((chunks, groups)),
        ],
        compiler_params=pltpu.CompilerParams(
            dimension_semantics=("arbitrary",), vmem_limit_bytes=63 * 1024 * 1024
        ),
        name="update_centroids",
    )(low, high, ids, prior, inverse, old, *[piece for part in parts for piece in part])


def two_level(rel, clusters):
    high = (rel // LANES)[:, None] == jnp.arange(clusters // LANES, dtype=jnp.int32)[None, :]
    low = (rel % LANES)[:, None] == jnp.arange(LANES, dtype=jnp.int32)[None, :]
    return high.astype(jnp.bfloat16), low


def spread(own, groups):
    pieces, hop = [own], groups // 2
    while hop > 0:
        pairs = [(source, source ^ hop) for source in range(groups)]
        more = []
        for piece in pieces:
            more.append(lax.ppermute(piece, "rep", pairs))
        pieces = pieces + more
        hop //= 2
    return pieces


def write_notes(rel, clusters, width, slabs):
    owners, cap = rel.shape
    upper = jnp.where(rel < 0, -1, jnp.where(rel < clusters, rel // DIGIT, DIGIT))
    lower = jnp.where((rel >= 0) & (rel < clusters), rel % DIGIT, 0)
    count = -(-cap // width)
    digits = [
        jnp.pad(part, ((0, 0), (0, count * width - cap))).reshape(owners, count, slabs, LANES)
        for part in (upper, lower)
    ]
    return jnp.concatenate(digits, axis=1).astype(jnp.bfloat16)


def read_notes(notes, cap):
    owners, _ = notes.shape[:2]
    digits = notes.astype(jnp.int32).reshape(owners, 2, -1)[:, :, :cap]
    return digits[:, 0] * DIGIT + digits[:, 1]


def on_device(embeddings, assignments, old_centroids, prior_counts):
    rows_here, width = embeddings.shape
    owners = lax.axis_size("rows")
    groups = lax.axis_size("rep")
    clusters = old_centroids.shape[0]
    assert clusters < DIGIT * DIGIT and groups & (groups - 1) == 0
    cap = 2 * rows_here // owners
    sizes = chunk_sizes(cap)
    chunks = len(sizes)
    begins = [sum(sizes[:c]) for c in range(chunks)]
    slabs = width // LANES

    owner = jnp.arange(owners, dtype=jnp.int32)
    bounds = owner * clusters
    starts = jnp.sum((assignments[None, :] < bounds[:, None]).astype(jnp.int32), axis=1)
    starts = jnp.minimum(starts, rows_here - cap)
    slot_row = (starts[:, None] + jnp.arange(cap, dtype=jnp.int32)[None, :]).reshape(-1)
    row = jnp.arange(rows_here, dtype=jnp.int32)
    slot_ids = jnp.sum(
        jnp.where(slot_row[:, None] == row[None, :], assignments[None, :], 0), axis=1
    ).reshape(owners, cap)
    notes = write_notes(slot_ids - bounds[:, None], clusters, width, slabs)

    rows3 = embeddings.reshape(rows_here, slabs, LANES)
    packed = list(pack_rows(starts, rows3, None, owners, begins[:1], sizes[:1]))
    packed += list(pack_rows(starts, rows3, notes, owners, begins[1:], sizes[1:]))
    pitches = [pack.shape[1] for pack in packed]

    parts = []
    for c in range(chunks):
        came = lax.all_to_all(packed[c], "rows", split_axis=0, concat_axis=0, tiled=True)
        pieces = spread(came, groups)
        if c == 1:
            noted = [piece[:, sizes[1] :] for piece in pieces]
        parts.append([piece.reshape(owners * pitches[c] * slabs, LANES) for piece in pieces])
    every = [read_notes(piece, cap) for piece in noted]
    rel = jnp.concatenate(every, axis=0)

    inside = (rel >= 0) & (rel < clusters)
    spots = jnp.where(inside, rel, clusters)
    spots = spots // ROWS * (ROWS * slabs) + spots % ROWS
    split = [rel[:, begins[c] : begins[c] + sizes[c]] for c in range(chunks)]
    spots = jnp.concatenate(
        [spots[:, begins[c] : begins[c] + sizes[c]].reshape(-1) for c in range(chunks)]
    )
    low = jnp.concatenate([jnp.sum((part < 0).astype(jnp.int32), axis=1) for part in split])
    high = jnp.concatenate([jnp.sum((part < clusters).astype(jnp.int32), axis=1) for part in split])

    flat = rel.reshape(-1)
    live = (flat >= 0) & (flat < clusters)
    hot_high, hot_low = two_level(jnp.where(live, flat, -1), clusters)
    counts = lax.dot_general(
        hot_high,
        (hot_low & live[:, None]).astype(jnp.bfloat16),
        (((0,), (0,)), ((), ())),
        preferred_element_type=jnp.float32,
    )
    prior = prior_counts.astype(jnp.float32).reshape(clusters // LANES, LANES)
    inverse = 1.0 / (prior + counts)

    mine = every[0].reshape(-1)
    mine_live = (mine >= 0) & (mine < clusters)
    my_high, my_low = two_level(jnp.where(mine_live, mine, 0), clusters)
    lanes = lax.dot_general(
        my_high,
        inverse.astype(jnp.bfloat16),
        (((1,), (0,)), ((), ())),
        preferred_element_type=jnp.float32,
    )
    my_weight = jnp.sum(jnp.where(my_low, lanes, 0.0), axis=1)

    centroids, partial = update(
        low, high, spots, prior, inverse, old_centroids, parts, owners, groups, sizes, pitches
    )

    dist = jnp.sum(partial, axis=1)
    dist = jnp.concatenate(
        [
            dist[owners * begins[c] : owners * (begins[c] + sizes[c])].reshape(owners, sizes[c])
            for c in range(chunks)
        ],
        axis=1,
    ).reshape(-1)
    scores = jnp.where(mine_live, my_weight * dist, 0.0).reshape(owners, cap)
    got = lax.all_to_all(scores, "rows", split_axis=0, concat_axis=0, tiled=True).reshape(-1)
    row_owner = assignments // clusters
    slot_owner = jnp.repeat(owner, cap)
    match = (slot_row[None, :] == row[:, None]) & (slot_owner[None, :] == row_owner[:, None])
    row_score = jnp.sum(jnp.where(match, got[None, :], 0.0), axis=1)
    return (centroids, row_score)


def solution(mesh):
    placed = (P(("rows", "rep"), None), P(("rows", "rep")), P("rows", None), P("rows"))
    return jax.shard_map(
        on_device,
        mesh=mesh,
        in_specs=placed,
        out_specs=(P("rows", None), P(("rows", "rep"))),
        check_vma=False,
    )
```
